256 devices in a mesh: wide: 64 (over x, y_hi, z), narrow: 4 (over y_lo, core).
Axes of the slice: x: 4, y: 4 (y_hi: 2, y_lo: 2; y = y_hi * 2 + y_lo), z: 8, core: 2. Of those that a mesh axis runs over, the one named last changes fastest.
Arguments:
- tokens: bfloat16 [8192, 2048], P('wide'), may hold values from -6 to 6
- expert_ids: int32 [8192, 6], P('wide'), may hold values from 0 to 63, all different within a row; in each aligned block of 128 rows (0 to 127, 128 to 255, ...) at most 16 rows name the same one
- gate_weights: float32 [8192, 6], P('wide'), may hold values from 0.05 to 0.6
- shared_gate: bfloat16 [2048, 2816], P('wide', 'narrow'), may hold values from -0.125 to 0.125
- shared_up: bfloat16 [2048, 2816], P('wide', 'narrow'), may hold values from -0.125 to 0.125
- shared_down: bfloat16 [2816, 2048], P('narrow', 'wide'), may hold values from -0.109375 to 0.109375
- expert_gate: bfloat16 [64, 2048, 1408], P('wide', None, 'narrow'), may hold values from -0.125 to 0.125
- expert_up: bfloat16 [64, 2048, 1408], P('wide', None, 'narrow'), may hold values from -0.125 to 0.125
- expert_down: bfloat16 [64, 1408, 2048], P('wide', 'narrow'), may hold values from -0.15625 to 0.15625
Outputs:
- moe_out: bfloat16 [8192, 2048], P('wide', 'narrow')
The draws below stay inside these ranges and needn't reach their ends.
Inputs may be any that keep to these rules, and one draw needn't show every extreme that they name: `expert_ids`: the 6 ids of a row differ. Among the 128 rows of one index of wide, no expert is named by more than 16 rows.
All inputs are finite; a program needn't handle non-finite values.
Results may differ from the reference program's by a relative error of at most 0.0075.
Values may be sent and summed in bfloat16 or wider, within the bound.
A program may use at most 128 MiB of HBM per device.

```python
import math
import jax
import jax.numpy as jnp
import numpy as np
from jax import lax

D = 2048
MF = 1408
FS = 2816
TOP = 6
TOK_DEV = 128
EXPERTS = 64
TOKENS = 8192
CAP = 16
N_WIDE = 64
N_NARROW = 4


def block_scale(stream_key, dims, split, low, high):
    def one(axis_at, blocks):
        steps = jax.random.uniform(jax.random.fold_in(jax.random.fold_in(stream_key, 6), axis_at), (blocks,), jnp.float32, low / len(split), high / len(split))
        return jnp.repeat(jnp.exp(steps), dims[axis_at] // blocks).reshape((-1,) + (1,) * (len(dims) - axis_at - 1))

    factor_of = one(*split[0])
    for cut in split[1:]:
        factor_of = factor_of * one(*cut)
    return factor_of


def shared_out(rng, own, number, rows, number_of, top, most, slope):
    ranking = jax.random.permutation(rng, number_of)
    packed, usual = load_shares(number_of, rows * top, most, slope, True), load_shares(number_of, rows * top, most, slope, False)
    places = jnp.arange(number_of)

    def named(lengths, offset_by):
        used = int((lengths > 0).sum())
        fixed = max(1, used // 4)
        passed = fixed + (places - fixed + offset_by * (used - fixed)) % max(1, number_of - fixed)
        return jnp.zeros((number_of,), jnp.int32).at[ranking[jnp.where(places < fixed, places, passed)]].set(jnp.asarray(lengths, jnp.int32))

    lengths = jnp.where(number % 4 == 0, named(packed, number // 4), named(usual, number - number // 4 - 1))
    mixed = jax.random.permutation(jax.random.fold_in(own, 3), number_of)
    donor, receiver = mixed[0:number_of // 2 * 2:2], mixed[1:number_of // 2 * 2:2]
    margin = jnp.minimum(lengths[donor] - 1, most - lengths[receiver]) // 2
    margin = jnp.where((donor == ranking[0]) | (receiver == ranking[0]) | (lengths[receiver] == 0), 0, jnp.maximum(margin, 0))
    passed = jax.random.randint(jax.random.fold_in(own, 4), (number_of // 2,), 0, 1 << 20) % (margin + 1)
    lengths = lengths.at[donor].add(-passed).at[receiver].add(passed)
    labels = jnp.searchsorted(jnp.cumsum(lengths), jnp.arange(rows * top), side="right").astype(jnp.int32)
    listing = labels.reshape(top, rows).T
    listing = listing[jax.random.permutation(jax.random.fold_in(own, 1), rows)]
    offset_by = jax.random.randint(jax.random.fold_in(own, 2), (rows, 1), 0, top)
    return jnp.take_along_axis(listing, (jnp.arange(top)[None, :] + offset_by) % top, axis=1)


def load_shares(amount, total, limit, lean, full):
    portions = [(1 << 20) // math.isqrt(grade ** lean) + 1 for grade in range(1, amount + 1)]
    largest = limit if full else min(limit, max(-(-total // amount), total * portions[0] // sum(portions)))
    least = 1 if total - largest >= amount - 1 else 0
    counts, surplus = [largest] + [least] * (amount - 1), total - largest - least * (amount - 1)
    while surplus > 0:
        candidates = [i for i in range(1, amount) if counts[i] < largest] or [i for i in range(1, amount) if counts[i] < limit]
        whole, budget = sum([portions[i] for i in candidates]), surplus
        for i in candidates:
            more = min(limit - counts[i], max(1, budget * portions[i] // whole), surplus)
            counts[i] = counts[i] + more
            surplus = surplus - more
    return np.array(counts)


def normal_values(stream_key, extent, spread, reach, cuts=(), held_as=jnp.bfloat16):
    array = jax.random.normal(stream_key, extent, jnp.float32) * spread
    if len(cuts) > 0:
        array = block_scale(stream_key, extent, cuts, -0.22, 0.18) * array
    return jnp.clip(array, min=-reach, max=reach).astype(held_as)


def setup_inputs(seed: int = 0) -> dict:
    keys = jax.random.split(jax.random.key(seed), 10)
    tokens = normal_values(keys[0], (TOKENS, D), 1.0, 6.0, ((0, 64),))
    expert_ids_keys = jax.random.split(jax.random.fold_in(keys[1], 1), TOKENS // TOK_DEV)
    expert_ids_turns = jax.random.permutation(jax.random.fold_in(keys[1], 3), TOKENS // TOK_DEV)
    expert_ids = jax.vmap(lambda own, number: shared_out(jax.random.fold_in(keys[1], 2), own, number, TOK_DEV, EXPERTS, TOP, CAP, 2))(expert_ids_keys, expert_ids_turns).reshape((TOKENS, TOP))
    gate_weights = jnp.clip(jnp.exp(math.log(0.6) - 2.4849067 * jax.random.uniform(keys[2], (TOKENS, TOP), jnp.float32) ** block_scale(keys[2], (TOKENS, TOP), ((0, 64),), -0.2, 0.2)), 0.05, 0.6)
    shared_gate = normal_values(keys[3], (D, FS), D ** -0.5, 0.125, ((0, 64), (1, 4)))
    shared_up = normal_values(keys[4], (D, FS), D ** -0.5, 0.125, ((0, 64), (1, 4)))
    shared_down = normal_values(keys[5], (FS, D), FS ** -0.5, 0.109375, ((0, 4), (1, 64)))
    expert_gate = normal_values(keys[6], (EXPERTS, D, MF), D ** -0.5, 0.125, ((0, 64), (2, 4)))
    expert_up = normal_values(keys[7], (EXPERTS, D, MF), D ** -0.5, 0.125, ((0, 64), (2, 4)))
    expert_down = normal_values(keys[8], (EXPERTS, MF, D), MF ** -0.5, 0.15625, ((0, 64), (1, 4)))
    return {"tokens": tokens, "expert_ids": expert_ids, "gate_weights": gate_weights, "shared_gate": shared_gate, "shared_up": shared_up, "shared_down": shared_down, "expert_gate": expert_gate, "expert_up": expert_up, "expert_down": expert_down}


def expert_rows(rows_in, w_gate, w_up, w_down):
    gate_part = jnp.dot(rows_in, w_gate, preferred_element_type=jnp.float32)
    up_part = jnp.dot(rows_in, w_up, preferred_element_type=jnp.float32)
    hidden = (jax.nn.silu(gate_part) * up_part).astype(jnp.bfloat16)
    quarter = MF // N_NARROW
    summed = jnp.zeros((rows_in.shape[0], w_down.shape[1]), jnp.float32)
    for slice_idx in range(N_NARROW):
        lower = slice_idx * quarter
        partial_value = jnp.dot(hidden[:, lower:lower + quarter], w_down[lower:lower + quarter], preferred_element_type=jnp.float32)
        summed = summed + partial_value.astype(jnp.bfloat16).astype(jnp.float32)
    return summed.astype(jnp.bfloat16)


def reference(tokens, expert_ids, gate_weights, shared_gate, shared_up, shared_down, expert_gate, expert_up, expert_down):
    shared_g = jnp.dot(tokens, shared_gate, preferred_element_type=jnp.float32)
    shared_u = jnp.dot(tokens, shared_up, preferred_element_type=jnp.float32)
    shared_hidden = (jax.nn.silu(shared_g) * shared_u).astype(jnp.bfloat16)
    shared = jnp.dot(shared_hidden, shared_down, preferred_element_type=jnp.float32)
    slot_count = N_WIDE * CAP
    positions = jnp.arange(TOKENS, dtype=jnp.int32)

    def one_expert(routed, inputs):
        expert_index, w_gate, w_up, w_down = inputs
        matches = expert_ids == expert_index
        chosen = jnp.any(matches, axis=1)
        weight = jnp.sum(jnp.where(matches, gate_weights, jnp.float32(0.0)), axis=1)
        rank_pos = (jnp.cumsum(chosen.astype(jnp.int32)) - 1).astype(jnp.int32)
        target = jnp.where(chosen, rank_pos, slot_count).astype(jnp.int32)
        picked = jnp.zeros((slot_count + 1,), jnp.int32).at[target].set(positions)[:slot_count]
        weight_live = jnp.zeros((slot_count + 1,), jnp.float32).at[target].set(weight)[:slot_count]
        outputs = expert_rows(tokens[picked], w_gate, w_up, w_down)
        routed = routed.at[picked].add(weight_live[:, None] * outputs.astype(jnp.float32))
        return routed, None

    routed0 = jnp.zeros((TOKENS, D), jnp.float32)
    indices = jnp.arange(EXPERTS, dtype=jnp.int32)
    routed, unused = lax.scan(one_expert, routed0, (indices, expert_gate, expert_up, expert_down))
    return (shared + routed).astype(jnp.bfloat16)
```

```python
import jax
import jax.numpy as jnp
from jax import lax
from jax.experimental import pallas as pl
from jax.experimental.pallas import tpu as pltpu
from jax.sharding import PartitionSpec as P

MESH = pl.DeviceIdType.MESH
BF16 = jnp.bfloat16
F32 = jnp.float32

NX, NY, NZ = 4, 2, 8
CAP = 16
GROUPS = NX * NY
ROWS = NZ * CAP
TOK = 128
D = 2048
Q = D // 4
H = 352
UNIT_ORDER = (0, 7, 1, 6, 2, 5, 3, 4)


def silu_mul(g, u):
    return (g * jax.nn.sigmoid(g) * u).astype(BF16)


def dot(a, b):
    return jnp.dot(a, b, preferred_element_type=F32)


def dot_t(a, b):
    return lax.dot_general(a, b, (((1,), (1,)), ((), ())), preferred_element_type=F32)


def kernel(
    tok, ids, gws, wp, eg, eu, ed, out,
    outg, full, wg, wu, wd, pbuf, r1, sbuf, keep, r2, fin, ret, whi, wlo, rank, gate, wall,
    ds_s, ds_r, a1_s, a1_r, a2_s, a2_r, b_s, b_r, r1_s, r1_r, r2_s, r2_r, rt_s, rt_r,
    w0_s, w0_r, zc_s, zc_r, zd_s, zd_r, xp_s, xp_r, xm_s, xm_r, xf_s, xf_r, xg_s, xg_r, l_s,
):
    w = lax.axis_index("wide")
    n = lax.axis_index("narrow")
    x, yh, z = w // (NY * NZ), (w // NZ) % NY, w % NZ
    a, c = n // 2, n % 2

    def dev(xx, yy, zz):
        return ((xx % NX) * NY + yy % NY) * NZ + zz % NZ

    mate = (w, 2 * a + 1 - c)
    over = (w, 2 * (1 - a) + c)
    n_mate, n_over, n_diag = mate[1], over[1], 2 * (1 - a) + 1 - c

    def remote(src, dst, ssem, rsem, device):
        return pltpu.make_async_remote_copy(
            src_ref=src, dst_ref=dst, send_sem=ssem, recv_sem=rsem,
            device_id=device, device_id_type=MESH,
        )

    def wait(ref, sem):
        pltpu.make_async_copy(ref, ref, sem).wait()

    barrier = pltpu.get_barrier_semaphore()

    def greet(d, carry):
        dx, dy, dz = d // (NY * NZ), (d // NZ) % NY, d % NZ
        pl.semaphore_signal(
            barrier, inc=1, device_id=(dev(x + dx, yh + dy, z + dz), n), device_id_type=MESH
        )
        return carry

    lax.fori_loop(1, NX * NY * NZ, greet, 0)
    pl.semaphore_signal(barrier, inc=1, device_id=mate, device_id_type=MESH)
    pl.semaphore_signal(barrier, inc=1, device_id=over, device_id_type=MESH)

    loads = (
        pltpu.make_async_copy(eg.at[0], wg, l_s.at[0]),
        pltpu.make_async_copy(eu.at[0], wu, l_s.at[1]),
        pltpu.make_async_copy(ed.at[0], wd, l_s.at[2]),
    )
    for load in loads:
        load.start()

    expert = lax.broadcasted_iota(jnp.int32, (NX * NY * NZ, TOK), 0)
    named = jnp.zeros((NX * NY * NZ, TOK), F32)
    weight = jnp.zeros((NX * NY * NZ, TOK), F32)
    for k in range(6):
        hit = ids[k : k + 1, :] == expert
        named = jnp.where(hit, 1.0, named)
        weight = jnp.where(hit, gws[k : k + 1, :], weight)
    upper = (
        lax.broadcasted_iota(jnp.int32, (TOK, TOK), 0)
        < lax.broadcasted_iota(jnp.int32, (TOK, TOK), 1)
    )
    before = dot(named.astype(BF16), jnp.where(upper, 1.0, 0.0).astype(BF16))
    rank[...] = jnp.where(named > 0.0, before, -1.0)
    gate[...] = weight
    wall[x, z, yh] = wp[yh]

    pl.semaphore_wait(barrier, NX * NY * NZ - 1 + 2)

    partner = (dev(x, yh + 1, z), n)
    w0 = remote(wp.at[1 - yh], wall.at[x, z, yh], w0_s, w0_r, partner)
    w0.start()
    to_partner = remote(
        tok.at[:, pl.ds(pl.multiple_of(n * Q, Q), Q)], full.at[GROUPS, n],
        ds_s.at[GROUPS, 0], ds_r.at[GROUPS, 0], partner,
    )

    slot = (lax.broadcasted_iota(jnp.int32, (ROWS, TOK), 0) % CAP).astype(F32)
    owner = lax.broadcasted_iota(jnp.int32, (ROWS, NZ), 0) // CAP
    spread = jnp.where(
        owner == lax.broadcasted_iota(jnp.int32, (ROWS, NZ), 1), 1.0, 0.0
    ).astype(BF16)

    def group_rank(g):
        e0 = pl.multiple_of(dev(x + g // NY, yh + g % NY, 0), NZ)
        return e0, dot(spread, rank[pl.ds(e0, NZ), :].astype(BF16)) == slot

    def send_copy(g, dz):
        zt = (z + dz) % NZ
        return remote(
            outg.at[g, pl.ds(zt * CAP, CAP)], full.at[g, n, pl.ds(z * CAP, CAP)],
            ds_s.at[g, dz], ds_r.at[g, dz], (dev(x + g // NY, yh + g % NY, zt), n),
        )

    def dispatch(g, carry):
        e0, hit = group_rank(g)
        pick = jnp.where(hit, 1.0, 0.0).astype(BF16)
        outg[g] = dot(pick, tok[:, pl.ds(pl.multiple_of(n * Q, Q), Q)]).astype(BF16)
        for dz in range(1, NZ):
            send_copy(g, dz).start()

        @pl.when(g > 0)
        def _():
            send_copy(g, 0).start()

        return carry

    lax.fori_loop(0, GROUPS, dispatch, 0)
    mine = pl.ds(z * CAP, CAP)
    full[0, n, mine] = outg[0, mine]
    to_partner.start()

    def weights(g, carry):
        e0, hit = group_rank(g)
        gw = gate[pl.ds(e0, NZ), :]
        gw_hi = gw.astype(BF16)
        gw_lo = (gw - gw_hi.astype(F32)).astype(BF16)
        zero = jnp.zeros((ROWS, TOK), F32)
        whi[g] = jnp.where(hit, dot(spread, gw_hi), zero).T.astype(BF16)
        wlo[g] = jnp.where(hit, dot(spread, gw_lo), zero).T.astype(BF16)
        return carry

    lax.fori_loop(0, GROUPS, weights, 0)

    def unit(xx, dz):
        return wall.at[xx % NX, (z + dz) % NZ]

    def x_send(dz):
        u = unit(x, dz)
        return (
            remote(u, u, xp_s.at[dz], xp_r.at[dz], (dev(x + 1, yh, z), n)),
            remote(u, u, xm_s.at[dz], xm_r.at[dz], (dev(x + NX - 1, yh, z), n)),
        )

    def x_forward(dz):
        lower = unit(x + NX - 1, dz).at[0]
        upper = unit(x + 1, dz).at[1]
        return (
            remote(lower, lower, xf_s.at[dz], xf_r.at[dz], (dev(x + 1, yh, z), n)),
            remote(upper, upper, xg_s.at[dz], xg_r.at[dz], (dev(x + NX - 1, yh, z), n)),
        )

    def z_send(s):
        up, down = unit(x, NZ - s), unit(x, s)
        if s == 3:
            up, down = up.at[0], down.at[1]
        return (
            remote(up, up, zc_s.at[s], zc_r.at[s], (dev(x, yh, z + 1), n)),
            remote(down, down, zd_s.at[s], zd_r.at[s], (dev(x, yh, z + NZ - 1), n)),
        )

    def ring(s):
        if s == 0:
            wait(wall.at[x, z, 1 - yh], w0_r)
        elif s < 4:
            wait(unit(x, NZ - s), zc_r.at[s - 1])
            wait(unit(x, s), zd_r.at[s - 1])
        else:
            wait(unit(x, 4).at[0], zc_r.at[3])
            wait(unit(x, 4).at[1], zd_r.at[3])
        if s < 4:
            for copy in z_send(s):
                copy.start()
        for dz in sorted({s, (NZ - s) % NZ}):
            for copy in x_send(dz):
                copy.start()

    def forward(dz):
        wait(unit(x + NX - 1, dz), xp_r.at[dz])
        wait(unit(x + 1, dz), xm_r.at[dz])
        for copy in x_forward(dz):
            copy.start()

    ring(0)
    for load in loads:
        load.wait()

    def gather_mate(i):
        return remote(full.at[i, n], full.at[i, n], a1_s.at[i], a1_r.at[i], mate)

    def gather_over(i):
        return remote(full.at[i, n], full.at[i, n], a2_s.at[i], a2_r.at[i], over)

    def gather_diag(i):
        return remote(full.at[i, n_over], full.at[i, n_over], b_s.at[i], b_r.at[i], mate)

    def scatter_mate(i):
        return remote(pbuf.at[i, 1 - c], r1.at[i], r1_s.at[i], r1_r.at[i], mate)

    def scatter_over(i):
        return remote(sbuf.at[i], r2.at[i], r2_s.at[i], r2_r.at[i], over)

    def return_copy(g, dz):
        zs = (z + NZ - dz) % NZ
        return remote(
            fin.at[g, pl.ds(zs * CAP, CAP)], ret.at[g, pl.ds(z * CAP, CAP)],
            rt_s.at[g, dz], rt_r.at[g, dz],
            (dev(x + NX - g // NY, yh + NY - g % NY, zs), n),
        )

    to_home = remote(fin.at[GROUPS], ret.at[GROUPS], rt_s.at[GROUPS, 0], rt_r.at[GROUPS, 0], partner)

    def arrive(i):
        @pl.when(i < GROUPS)
        def _():
            for dz in range(1, NZ):
                wait(full.at[i, n, pl.ds(((z + NZ - dz) % NZ) * CAP, CAP)], ds_r.at[i, dz])

            @pl.when(i > 0)
            def _():
                wait(full.at[i, n, mine], ds_r.at[i, 0])

        @pl.when(i == GROUPS)
        def _():
            wait(full.at[GROUPS, n], ds_r.at[GROUPS, 0])

        gather_over(i).start()
        gather_mate(i).start()

    def pass_on(i):
        wait(full.at[i, n_over], a2_r.at[i])
        gather_diag(i).start()

    def gathered(i):
        wait(full.at[i, n_mate], a1_r.at[i])
        wait(full.at[i, n_diag], b_r.at[i])

    def ffn(i):
        gathered(i)
        gp = jnp.zeros((ROWS, H), F32)
        up = jnp.zeros((ROWS, H), F32)
        for q in range(4):
            rows = full[i, q]
            gp += dot(rows, wg[q * Q : (q + 1) * Q, :])
            up += dot(rows, wu[q * Q : (q + 1) * Q, :])
        hidden = silu_mul(gp, up)
        for q in range(4):
            pbuf[i, q % 2, q // 2] = dot(hidden, wd[:, q * Q : (q + 1) * Q]).astype(BF16)
        scatter_mate(i).start()

    def add_mate(i):
        wait(r1.at[i], r1_r.at[i])
        sbuf[i] = (pbuf[i, c, 1 - a].astype(F32) + r1[i, 1 - a].astype(F32)).astype(BF16)
        scatter_over(i).start()
        keep[i] = pbuf[i, c, a].astype(F32) + r1[i, a].astype(F32)

    def add_over(i):
        wait(r2.at[i], r2_r.at[i])
        return keep[i] + r2[i].astype(F32)

    def send_home(i):
        fin[i] = add_over(i).astype(BF16)
        for dz in range(1, NZ):
            return_copy(i, dz).start()

        @pl.when(i > 0)
        def _():
            return_copy(i, 0).start()

        @pl.when(i == 0)
        def _():
            ret[0, mine] = fin[0, mine]

    side = {1: [lambda: ring(1)], 3: [lambda: ring(2)], 5: [lambda: ring(3)], 7: [lambda: ring(4)]}
    for it, dzs in {2: (0,), 4: (7, 1), 6: (6, 2), 8: (5, 3), 10: (4,)}.items():
        side.setdefault(it, []).extend([lambda dz=dz: forward(dz) for dz in dzs])

    def step(i, carry):
        @pl.when(i <= GROUPS)
        def _():
            arrive(i)

        @pl.when((i >= 1) & (i <= GROUPS + 1))
        def _():
            pass_on(i - 1)

        @pl.when((i >= 2) & (i < GROUPS + 2))
        def _():
            ffn(i - 2)

        @pl.when((i >= 3) & (i < GROUPS + 3))
        def _():
            add_mate(i - 3)

        @pl.when((i >= 4) & (i < GROUPS + 4))
        def _():
            send_home(i - 4)

        for it, jobs in side.items():
            @pl.when(i == it)
            def _():
                for job in jobs:
                    job()

        return carry

    lax.fori_loop(0, GROUPS + 4, step, 0)

    for dz in range(NZ):
        wait(unit(x + 2, dz).at[0], xf_r.at[dz])
        wait(unit(x + 2, dz).at[1], xg_r.at[dz])
    gathered(GROUPS)
    gp = jnp.zeros((2 * TOK, H), F32)
    up = jnp.zeros((2 * TOK, H), F32)
    wide_block = NZ * 32
    for k in range(NX * NY):
        xx, yy = k // NY, k % NY
        rows = jnp.concatenate(
            [
                full[GROUPS, xx, :, yy * wide_block : (yy + 1) * wide_block],
                tok[:, k * wide_block : (k + 1) * wide_block],
            ],
            axis=0,
        )
        gp += dot(rows, wall[xx, :, yy, 0].reshape(wide_block, H))
        up += dot(rows, wall[xx, :, yy, 1].reshape(wide_block, H))
    hidden = silu_mul(gp, up)
    for k in range(NX * NY):
        xx, yy = k // NY, k % NY
        part = dot_t(hidden, wall[xx, :, yy, 2].reshape(wide_block, H)).astype(BF16)
        cols = slice(yy * wide_block, (yy + 1) * wide_block)
        pbuf[GROUPS, xx % 2, xx // 2, :, cols] = part[:TOK]
        pbuf[GROUPS + 1, xx % 2, xx // 2, :, cols] = part[TOK:]
    scatter_mate(GROUPS).start()
    scatter_mate(GROUPS + 1).start()

    def combine(lo, hi, acc):
        for g in range(lo, hi):
            for dz in range(1 if g == 0 else 0, NZ):
                wait(ret.at[g, pl.ds(((z + dz) % NZ) * CAP, CAP)], rt_r.at[g, dz])
            acc = acc + dot(whi[g], ret[g]) + dot(wlo[g], ret[g])
        return acc

    acc = combine(0, GROUPS // 2, jnp.zeros((TOK, Q), F32))
    add_mate(GROUPS)
    add_mate(GROUPS + 1)
    acc = combine(GROUPS // 2, GROUPS, acc)
    fin[GROUPS] = add_over(GROUPS).astype(BF16)
    to_home.start()
    acc = acc + add_over(GROUPS + 1)
    wait(ret.at[GROUPS], rt_r.at[GROUPS, 0])
    out[...] = (acc + ret[GROUPS].astype(F32)).astype(BF16)

    w0.wait_send()
    to_partner.wait_send()
    to_home.wait_send()

    def drain(g, carry):
        for dz in range(1, NZ):
            send_copy(g, dz).wait_send()
            return_copy(g, dz).wait_send()

        @pl.when(g > 0)
        def _():
            send_copy(g, 0).wait_send()
            return_copy(g, 0).wait_send()

        return carry

    lax.fori_loop(0, GROUPS, drain, 0)

    def drain_narrow(i, carry):
        gather_over(i).wait_send()
        gather_mate(i).wait_send()
        gather_diag(i).wait_send()
        scatter_mate(i).wait_send()
        scatter_over(i).wait_send()
        return carry

    lax.fori_loop(0, GROUPS + 1, drain_narrow, 0)
    scatter_mate(GROUPS + 1).wait_send()
    scatter_over(GROUPS + 1).wait_send()
    for s in range(4):
        for copy in z_send(s):
            copy.wait_send()

    def drain_x(dz, carry):
        for copy in x_send(dz) + x_forward(dz):
            copy.wait_send()
        return carry

    lax.fori_loop(0, NZ, drain_x, 0)


def layer(tok, ids, gws, wp, eg, eu, ed):
    vmem = pl.BlockSpec(memory_space=pltpu.VMEM)
    hbm = pl.BlockSpec(memory_space=pl.ANY)
    dma = pltpu.SemaphoreType.DMA
    G = GROUPS
    return pl.pallas_call(
        kernel,
        out_shape=jax.ShapeDtypeStruct((TOK, Q), BF16),
        in_specs=[vmem, vmem, vmem, vmem, hbm, hbm, hbm],
        out_specs=vmem,
        scratch_shapes=[
            pltpu.VMEM((G, ROWS, Q), BF16),
            pltpu.VMEM((G + 1, 4, ROWS, Q), BF16),
            pltpu.VMEM((D, H), BF16),
            pltpu.VMEM((D, H), BF16),
            pltpu.VMEM((H, D), BF16),
            pltpu.VMEM((G + 2, 2, 2, ROWS, Q), BF16),
            pltpu.VMEM((G + 2, 2, ROWS, Q), BF16),
            pltpu.VMEM((G + 2, ROWS, Q), BF16),
            pltpu.VMEM((G + 2, ROWS, Q), F32),
            pltpu.VMEM((G + 2, ROWS, Q), BF16),
            pltpu.VMEM((G + 1, ROWS, Q), BF16),
            pltpu.VMEM((G + 1, ROWS, Q), BF16),
            pltpu.VMEM((G, TOK, ROWS), BF16),
            pltpu.VMEM((G, TOK, ROWS), BF16),
            pltpu.VMEM((NX * NY * NZ, TOK), F32),
            pltpu.VMEM((NX * NY * NZ, TOK), F32),
            pltpu.VMEM((NX, NZ, NY, 3, 32, H), BF16),
            dma((G + 1, NZ)), dma((G + 1, NZ)),
            dma((G + 1,)), dma((G + 1,)), dma((G + 1,)), dma((G + 1,)), dma((G + 1,)), dma((G + 1,)),
            dma((G + 2,)), dma((G + 2,)), dma((G + 2,)), dma((G + 2,)),
            dma((G + 1, NZ)), dma((G + 1, NZ)),
            dma, dma,
            dma((4,)), dma((4,)), dma((4,)), dma((4,)),
            dma((NZ,)), dma((NZ,)), dma((NZ,)), dma((NZ,)),
            dma((NZ,)), dma((NZ,)), dma((NZ,)), dma((NZ,)),
            dma((3,)),
        ],
        compiler_params=pltpu.CompilerParams(
            collective_id=0, has_side_effects=True, vmem_limit_bytes=62 * 1024 * 1024
        ),
    )(tok, ids, gws, wp, eg, eu, ed)


def body(tokens, expert_ids, gate_weights, shared_gate, shared_up, shared_down,
         expert_gate, expert_up, expert_down):
    pad = ((0, 2), (0, 0))
    ids = jnp.pad(expert_ids.T, pad)
    gws = jnp.pad(gate_weights.T, pad)
    packed = jnp.stack([shared_gate, shared_up, shared_down.T])
    packed = packed.reshape(3, 32, NY, H).transpose(2, 0, 1, 3)
    return layer(tokens, ids, gws, packed, expert_gate, expert_up, expert_down)


def solution(mesh):
    in_specs = (
        P("wide", None), P("wide", None), P("wide", None),
        P("wide", "narrow"), P("wide", "narrow"), P("narrow", "wide"),
        P("wide", None, "narrow"), P("wide", None, "narrow"), P("wide", "narrow", None),
    )
    return jax.shard_map(
        body, mesh=mesh, in_specs=in_specs, out_specs=P("wide", "narrow"), check_vma=False
    )
```

```python
import jax
import jax.numpy as jnp
from jax import lax
from jax.experimental import pallas as pl
from jax.experimental.pallas import tpu as pltpu
from jax.sharding import PartitionSpec as P

MESH = pl.DeviceIdType.MESH
BF16 = jnp.bfloat16
F32 = jnp.float32

NX, NY, NZ = 4, 2, 8
CAP = 16
GROUPS = NX * NY
ROWS = NZ * CAP
TOK = 128
D = 2048
Q = D // 4
H = 352
ORDER = (0, 7, 1, 6, 2, 5, 3, 4)
UNITS = (0, 7, 1, 6, 2, 5, 3, 4)
LAG = (2, 3, 4, 5, 6, 8)
TOKEN_RING = (1, 2, 3, 4)
RING = (1, 3, 4, 6, 7)
X_SEND = (1, 3, 4, 5, 6, 7, 8, 8)
FORWARD = (4, 6, 7, 8, 9, 10, 11, 12)
SHARED = 13


def silu_mul(g, u):
    return (g * jax.nn.sigmoid(g) * u).astype(BF16)


def dot(a, b):
    return jnp.dot(a, b, preferred_element_type=F32)


def dot_t(a, b):
    return lax.dot_general(a, b, (((1,), (1,)), ((), ())), preferred_element_type=F32)


def kernel(
    tok, ids, gws, sg, su, sd, eg, eu, ed, out,
    wp, mine, mg, tblk, outg, full, wg, wu, wd, pbuf, r1, sbuf, keep, r2, fin, ret, zout, zin,
    whi, wlo, own, wall,
    mg_s, mg_r, tp_s, th_s, tc_s, tc_r, td_s, td_r,
    ds_s, ds_r, a1_s, a1_r, a2_s, a2_r, b_s, b_r, r1_s, r1_r, r2_s, r2_r, rt_s, rt_r, zr_s, zr_r,
    w0_s, w0_r, zc_s, zc_r, zd_s, zd_r, xp_s, xp_r, xm_s, xm_r, xf_s, xf_r, xg_s, xg_r, l_s,
):
    w = lax.axis_index("wide")
    n = lax.axis_index("narrow")
    x, yh, z = w // (NY * NZ), (w // NZ) % NY, w % NZ
    a, c = n // 2, n % 2

    def dev(xx, yy, zz):
        return ((xx % NX) * NY + yy % NY) * NZ + zz % NZ

    mate = (w, 2 * a + 1 - c)
    over = (w, 2 * (1 - a) + c)
    n_mate, n_over, n_diag = mate[1], over[1], 2 * (1 - a) + 1 - c
    partner = (dev(x, yh + 1, z), n)

    def peer(dx, dy, back=False):
        if back:
            dx, dy = NX - dx, NY - dy
        return (dev(x + dx, yh + dy, z), n if dy % NY == 0 else n_over)

    def remote(src, dst, ssem, rsem, device):
        return pltpu.make_async_remote_copy(
            src_ref=src, dst_ref=dst, send_sem=ssem, recv_sem=rsem,
            device_id=device, device_id_type=MESH,
        )

    def wait(ref, sem):
        pltpu.make_async_copy(ref, ref, sem).wait()

    barrier = pltpu.get_barrier_semaphore()
    friends = [peer(j % NX, j // NX) for j in range(1, GROUPS)]
    friends += [(dev(x, yh, z + dz), n) for dz in range(1, NZ)]
    friends += [mate, over, partner]
    for friend in friends:
        pl.semaphore_signal(barrier, inc=1, device_id=friend, device_id_type=MESH)

    loads = (
        pltpu.make_async_copy(eg.at[0], wg, l_s.at[0]),
        pltpu.make_async_copy(eu.at[0], wu, l_s.at[1]),
        pltpu.make_async_copy(ed.at[0], wd, l_s.at[2]),
    )
    for load in loads:
        load.start()

    for k, shard in enumerate((sg, su, sd)):
        for half in range(NY):
            wp[half, k] = shard[:, half * H : (half + 1) * H]
    wall[x, z, yh] = wp[yh]
    quarter = pl.ds(pl.multiple_of(n * Q, Q), Q)
    tblk[z] = tok[:, quarter]
    mine[:6] = ids[...].astype(F32)
    mine[8:14] = gws[...]
    mg[z] = mine[...]
    upper = jnp.where(
        lax.broadcasted_iota(jnp.int32, (TOK, TOK), 0)
        < lax.broadcasted_iota(jnp.int32, (TOK, TOK), 1),
        1.0, 0.0,
    ).astype(BF16)
    row = lax.broadcasted_iota(jnp.int32, (ROWS, GROUPS), 0) // CAP
    spread = jnp.where(
        (((x + row % NX) % NX) * NY + (yh + row // NX) % NY)
        == lax.broadcasted_iota(jnp.int32, (ROWS, GROUPS), 1),
        1.0, 0.0,
    ).astype(BF16)
    slot = (lax.broadcasted_iota(jnp.int32, (ROWS, TOK), 0) % CAP).astype(F32)
    expert = (lax.broadcasted_iota(jnp.int32, (GROUPS, TOK), 0) * NZ + z).astype(F32)

    pl.semaphore_wait(barrier, len(friends))

    w0 = remote(wp.at[1 - yh], wall.at[x, z, yh], w0_s, w0_r, partner)
    w0.start()

    def meta_send(dz):
        return remote(mine, mg.at[z], mg_s, mg_r.at[dz], (dev(x, yh, z + dz), n))

    def block(dz):
        return tblk.at[(z + dz) % NZ]

    def token_send(s):
        up, down = block(NZ - s), block(s)
        up_src, down_src = up, down
        if s == 0:
            up_src = down_src = tok.at[:, quarter]
        if s == 3:
            up_src = up = up.at[: TOK // 2]
            down_src = down = down.at[TOK // 2 :]
        return (
            remote(up_src, up, tc_s.at[s], tc_r.at[s], (dev(x, yh, z + 1), n)),
            remote(down_src, down, td_s.at[s], td_r.at[s], (dev(x, yh, z + NZ - 1), n)),
        )

    def token_ring(s):
        if s < 4:
            wait(block(NZ - s), tc_r.at[s - 1])
            wait(block(s), td_r.at[s - 1])
            for copy in token_send(s):
                copy.start()
        else:
            wait(block(4).at[: TOK // 2], tc_r.at[3])
            wait(block(4).at[TOK // 2 :], td_r.at[3])

    for copy in token_send(0):
        copy.start()
    for dz in range(1, NZ):
        meta_send(dz).start()
    to_partner = remote(
        tok.at[:, quarter], full.at[GROUPS, n_over],
        tp_s, ds_r.at[GROUPS], (partner[0], n_over),
    )

    def offset(k):
        early = (k + 1) // 2 * (1 - k % 2 * 2)
        late = 4 - (k - 4) // 2 + k % 2 * (1 - (k - 4) // 2 * 2)
        return (early * ((7 - k) // 4) + late * (k // 4) + NZ) % NZ

    def part_of(j):
        return pl.ds(j * CAP, CAP)

    def row_send(k, j):
        return remote(
            outg.at[k, part_of(j)], full.at[k, peer(j % NX, j // NX)[1], part_of(j)],
            ds_s, ds_r.at[k], peer(j % NX, j // NX),
        )

    def select(k):
        zb = (z + offset(k)) % NZ

        @pl.when(k > 0)
        def _():
            dz = (NZ - offset(k)) % NZ
            wait(mg.at[zb], mg_r.at[dz])

        named = jnp.zeros((GROUPS, TOK), F32)
        weight = jnp.zeros((GROUPS, TOK), F32)
        for t in range(6):
            hit = mg[zb, t : t + 1, :] == expert
            named = jnp.where(hit, 1.0, named)
            weight = jnp.where(hit, mg[zb, 8 + t : 9 + t, :], weight)
        before = dot(named.astype(BF16), upper)
        rank = jnp.where(named > 0.0, before, -1.0)
        hit = dot(spread, rank.astype(BF16)) == slot
        outg[k] = dot(jnp.where(hit, 1.0, 0.0).astype(BF16), tblk[zb]).astype(BF16)
        for j in range(1, GROUPS):
            row_send(k, j).start()
        full[k, n, :CAP] = outg[k, :CAP]
        w_hi = weight.astype(BF16)
        w_lo = (weight - w_hi.astype(F32)).astype(BF16)
        zero = jnp.zeros((ROWS, TOK), F32)
        whi[k] = jnp.where(hit, dot(spread, w_hi), zero).T.astype(BF16)
        wlo[k] = jnp.where(hit, dot(spread, w_lo), zero).T.astype(BF16)

    def unit(xx, dz):
        return wall.at[xx % NX, (z + dz) % NZ]

    def x_send(dz):
        u = unit(x, dz)
        return (
            remote(u, u, xp_s, xp_r.at[dz], (dev(x + 1, yh, z), n)),
            remote(u, u, xm_s, xm_r.at[dz], (dev(x + NX - 1, yh, z), n)),
        )

    def x_forward(dz):
        lower = unit(x + NX - 1, dz).at[0]
        upper = unit(x + 1, dz).at[1]
        return (
            remote(lower, lower, xf_s, xf_r, (dev(x + 1, yh, z), n)),
            remote(upper, upper, xg_s, xg_r, (dev(x + NX - 1, yh, z), n)),
        )

    def z_send(s):
        up, down = unit(x, NZ - s), unit(x, s)
        if s == 3:
            up, down = up.at[0], down.at[1]
        return (
            remote(up, up, zc_s.at[s], zc_r.at[s], (dev(x, yh, z + 1), n)),
            remote(down, down, zd_s.at[s], zd_r.at[s], (dev(x, yh, z + NZ - 1), n)),
        )

    def ring(s):
        if s == 0:
            wait(wall.at[x, z, 1 - yh], w0_r)
        elif s < 4:
            wait(unit(x, NZ - s), zc_r.at[s - 1])
            wait(unit(x, s), zd_r.at[s - 1])
        else:
            wait(unit(x, 4).at[0], zc_r.at[3])
            wait(unit(x, 4).at[1], zd_r.at[3])
        if s < 4:
            for copy in z_send(s):
                copy.start()

    def forward(dz):
        wait(unit(x + NX - 1, dz), xp_r.at[dz])
        wait(unit(x + 1, dz), xm_r.at[dz])
        for copy in x_forward(dz):
            copy.start()

    to_partner.start()
    for load in loads:
        load.wait()

    def gather_mate(i):
        return remote(full.at[i, n], full.at[i, n], a1_s, a1_r.at[i], mate)

    def gather_over(i):
        return remote(full.at[i, n], full.at[i, n], a2_s, a2_r.at[i], over)

    def gather_diag(i):
        return remote(full.at[i, n_over], full.at[i, n_over], b_s, b_r.at[i], mate)

    def scatter_mate(i):
        return remote(pbuf.at[i, 1 - c], r1.at[i], r1_s, r1_r.at[i], mate)

    def scatter_over(i):
        return remote(sbuf.at[i], r2.at[i], r2_s, r2_r.at[i], over)

    def return_copy(k, j):
        return remote(
            fin.at[k, part_of(j)], ret.at[k, part_of(j)],
            rt_s, rt_r.at[k], peer(j % NX, j // NX, back=True),
        )

    to_home = remote(
        fin.at[GROUPS], ret.at[GROUPS], th_s, rt_r.at[GROUPS],
        (partner[0], n_over),
    )

    def arrive(i):
        @pl.when(i < GROUPS)
        def _():
            wait(full.at[i, n, pl.ds(CAP, ROWS - CAP)], ds_r.at[i])

        @pl.when(i == GROUPS)
        def _():
            wait(full.at[GROUPS, n], ds_r.at[GROUPS])

        gather_over(i).start()
        gather_mate(i).start()

    def pass_on(i):
        wait(full.at[i, n_over], a2_r.at[i])
        gather_diag(i).start()

    def gathered(i):
        wait(full.at[i, n_mate], a1_r.at[i])
        wait(full.at[i, n_diag], b_r.at[i])

    half = ROWS // 2

    def ffn(i):
        gathered(i)
        gp = jnp.zeros((ROWS, H), F32)
        up = jnp.zeros((ROWS, H), F32)
        for q in range(4):
            rows = jnp.concatenate([full[i, q, :half], full[i, (q + 2) % 4, half:]], axis=0)
            gp += dot_t(rows, wg[:, q * Q : (q + 1) * Q])
            up += dot_t(rows, wu[:, q * Q : (q + 1) * Q])
        hidden = silu_mul(gp, up)
        for q in range(4):
            part = dot(hidden, wd[:, q * Q : (q + 1) * Q]).astype(BF16)
            pbuf[i, q % 2, q // 2, :half] = part[:half]
            pbuf[i, q % 2, 1 - q // 2, half:] = part[half:]
        scatter_mate(i).start()

    def add_mate(i):
        wait(r1.at[i], r1_r.at[i])
        sbuf[i] = (pbuf[i, c, 1 - a].astype(F32) + r1[i, 1 - a].astype(F32)).astype(BF16)
        scatter_over(i).start()
        keep[i] = pbuf[i, c, a].astype(F32) + r1[i, a].astype(F32)

    def add_over(i):
        wait(r2.at[i], r2_r.at[i])
        return keep[i] + r2[i].astype(F32)

    def send_home(i):
        fin[i] = add_over(i).astype(BF16)
        for j in range(1, GROUPS):
            return_copy(i, j).start()
        ret[i, :CAP] = fin[i, :CAP]

    def z_return(k):
        return remote(
            zout.at[k], zin.at[k], zr_s, zr_r.at[k], (dev(x, yh, z + offset(k)), n)
        )

    def combine(k):
        wait(ret.at[k, pl.ds(CAP, ROWS - CAP)], rt_r.at[k])
        part = dot(whi[k], ret[k]) + dot(wlo[k], ret[k])

        @pl.when(k == 0)
        def _():
            own[...] = part

        @pl.when(k > 0)
        def _():
            zout[k] = part.astype(BF16)
            z_return(k).start()

    def shared():
        wait(wall.at[0, : NZ // 2], xf_r)
        wait(wall.at[0, : NZ // 2], xg_r)
        gathered(GROUPS)
        gp = jnp.zeros((2 * TOK, H), F32)
        up = jnp.zeros((2 * TOK, H), F32)
        wide_block = NZ * 32
        for k in range(NX * NY):
            xx, yy = k // NY, k % NY
            rows = jnp.concatenate(
                [
                    full[GROUPS, (xx + 2) % 4, :, yy * wide_block : (yy + 1) * wide_block],
                    tok[:, k * wide_block : (k + 1) * wide_block],
                ],
                axis=0,
            )
            gp += dot(rows, wall[xx, :, yy, 0].reshape(wide_block, H))
            up += dot(rows, wall[xx, :, yy, 1].reshape(wide_block, H))
        hidden = silu_mul(gp, up)
        for k in range(NX * NY):
            xx, yy = k // NY, k % NY
            part = dot_t(hidden, wall[xx, :, yy, 2].reshape(wide_block, H)).astype(BF16)
            cols = slice(yy * wide_block, (yy + 1) * wide_block)
            pbuf[GROUPS, xx % 2, 1 - xx // 2, :, cols] = part[:TOK]
            pbuf[GROUPS + 1, xx % 2, xx // 2, :, cols] = part[TOK:]
        scatter_mate(GROUPS).start()
        scatter_mate(GROUPS + 1).start()

    side = {}
    for k, it in enumerate(RING):
        side.setdefault(it, []).append(lambda k=k: ring(k))
    for k in range(NZ):
        side.setdefault(X_SEND[k], []).append(lambda k=k: [c.start() for c in x_send(UNITS[k])])
        side.setdefault(FORWARD[k], []).append(lambda k=k: forward(UNITS[k]))
    side.setdefault(SHARED, []).append(shared)
    side.setdefault(SHARED + 1, []).extend([lambda: add_mate(GROUPS), lambda: add_mate(GROUPS + 1)])

    def step(i, carry):
        for k, it in enumerate(TOKEN_RING):
            @pl.when(i == it)
            def _():
                token_ring(k + 1)

        stages = (
            (0, GROUPS, select), (LAG[0], GROUPS + 1, arrive), (LAG[1], GROUPS + 1, pass_on),
            (LAG[2], GROUPS, ffn), (LAG[3], GROUPS, add_mate), (LAG[4], GROUPS, send_home),
            (LAG[5], GROUPS, combine),
        )
        for lag, count, stage in stages:
            @pl.when((i >= lag) & (i < count + lag))
            def _():
                stage(i - lag)

        for it, jobs in side.items():
            @pl.when(i == it)
            def _():
                for job in jobs:
                    job()

        return carry

    lax.fori_loop(0, GROUPS + LAG[5], step, 0)

    fin[GROUPS] = add_over(GROUPS).astype(BF16)
    to_home.start()
    acc = own[...]
    for k in range(1, GROUPS):
        wait(zin.at[k], zr_r.at[k])
        acc += zin[k].astype(F32)
    acc = acc + add_over(GROUPS + 1)
    wait(ret.at[GROUPS], rt_r.at[GROUPS])
    out[...] = (acc + ret[GROUPS].astype(F32)).astype(BF16)

    w0.wait_send()
    to_partner.wait_send()
    to_home.wait_send()
    wait(outg.at[: GROUPS - 1], ds_s)
    wait(outg.at[: GROUPS - 1], rt_s)
    wait(outg.at[: GROUPS - 1], zr_s)
    wait(mg.at[: NZ - 1], mg_s)
    for sem in (a1_s, a2_s, b_s):
        wait(full.at[:, 0], sem)
    wait(r1, r1_s)
    wait(r2, r2_s)
    wait(wall.at[0], xp_s)
    wait(wall.at[0], xm_s)
    wait(wall.at[0, : NZ // 2], xf_s)
    wait(wall.at[0, : NZ // 2], xg_s)
    for s in range(4):
        for copy in token_send(s) + z_send(s):
            copy.wait_send()


def layer(tok, ids, gws, sg, su, sd, eg, eu, ed):
    vmem = pl.BlockSpec(memory_space=pltpu.VMEM)
    hbm = pl.BlockSpec(memory_space=pl.ANY)
    dma = pltpu.SemaphoreType.DMA
    G = GROUPS
    return pl.pallas_call(
        kernel,
        out_shape=jax.ShapeDtypeStruct((TOK, Q), BF16),
        in_specs=[vmem] * 6 + [hbm] * 3,
        out_specs=vmem,
        scratch_shapes=[
            pltpu.VMEM((NY, 3, 32, H), BF16),
            pltpu.VMEM((16, TOK), F32),
            pltpu.VMEM((NZ, 16, TOK), F32),
            pltpu.VMEM((NZ, TOK, Q), BF16),
            pltpu.VMEM((G, ROWS, Q), BF16),
            pltpu.VMEM((G + 1, 4, ROWS, Q), BF16),
            pltpu.VMEM((H, D), BF16),
            pltpu.VMEM((H, D), BF16),
            pltpu.VMEM((H, D), BF16),
            pltpu.VMEM((G + 2, 2, 2, ROWS, Q), BF16),
            pltpu.VMEM((G + 2, 2, ROWS, Q), BF16),
            pltpu.VMEM((G + 2, ROWS, Q), BF16),
            pltpu.VMEM((G + 2, ROWS, Q), F32),
            pltpu.VMEM((G + 2, ROWS, Q), BF16),
            pltpu.VMEM((G + 1, ROWS, Q), BF16),
            pltpu.VMEM((G + 1, ROWS, Q), BF16),
            pltpu.VMEM((G, TOK, Q), BF16),
            pltpu.VMEM((G, TOK, Q), BF16),
            pltpu.VMEM((G, TOK, ROWS), BF16),
            pltpu.VMEM((G, TOK, ROWS), BF16),
            pltpu.VMEM((TOK, Q), F32),
            pltpu.VMEM((NX, NZ, NY, 3, 32, H), BF16),
            dma, dma((NZ,)), dma, dma,
            dma((4,)), dma((4,)), dma((4,)), dma((4,)),
            dma, dma((G + 1,)), dma, dma((G + 1,)), dma, dma((G + 1,)), dma, dma((G + 1,)),
            dma, dma((G + 2,)), dma, dma((G + 2,)), dma, dma((G + 1,)), dma, dma((G,)),
            dma, dma, dma((4,)), dma((4,)), dma((4,)), dma((4,)),
            dma, dma((NZ,)), dma, dma((NZ,)), dma, dma, dma, dma,
            dma((3,)),
        ],
        compiler_params=pltpu.CompilerParams(
            collective_id=0, has_side_effects=True, vmem_limit_bytes=62 * 1024 * 1024
        ),
    )(tok, ids, gws, sg, su, sd, eg, eu, ed)


def body(tokens, expert_ids, gate_weights, shared_gate, shared_up, shared_down,
         expert_gate, expert_up, expert_down):
    return layer(
        tokens, expert_ids.T, gate_weights.T, shared_gate, shared_up, shared_down.T,
        jnp.swapaxes(expert_gate, 1, 2), jnp.swapaxes(expert_up, 1, 2), expert_down,
    )


def solution(mesh):
    in_specs = (
        P("wide", None), P("wide", None), P("wide", None),
        P("wide", "narrow"), P("wide", "narrow"), P("narrow", "wide"),
        P("wide", None, "narrow"), P("wide", None, "narrow"), P("wide", "narrow", None),
    )
    return jax.shard_map(
        body, mesh=mesh, in_specs=in_specs, out_specs=P("wide", "narrow"), check_vma=False
    )
```

```python
import jax
import jax.numpy as jnp
from jax import lax
from jax.experimental import pallas as pl
from jax.experimental.pallas import tpu as pltpu
from jax.sharding import PartitionSpec as P

MESH = pl.DeviceIdType.MESH
BF16 = jnp.bfloat16
F32 = jnp.float32

NX, NY, NZ = 4, 2, 8
CAP = 16
GROUPS = NX * NY
ROWS = NZ * CAP
TOK = 128
D = 2048
Q = D // 4
H = 352
ORDER = (0, 7, 1, 6, 2, 5, 3, 4)
UNITS = (0, 7, 1, 6, 2, 5, 3, 4)
ORDER = (0, 7, 6, 4, 3, 5, 2, 1)
TOKEN_RING = (2, 4, 5, 6)
SELECT = (0, 2, 4, 6, 5, 5, 4, 2)
ARRIVE = (1, 4, 5, 7, 6, 6, 5, 4, 7)
PASS_ON = (5, 6, 8, 7, 7, 6, 5)
FIRST = (3, 4, 5, 7)
LAG = (5, 6, 7, 8)
RING = (2, 4, 5, 6, 8)
X_SEND = (2, 4, 5, 6, 7, 8, 9, 10)
FORWARD = (5, 7, 8, 9, 10, 11, 12, 13)
SHARED = 14
PARTNER = 4


def silu_mul(g, u):
    return (g * jax.nn.sigmoid(g) * u).astype(BF16)


def dot(a, b):
    return jnp.dot(a, b, preferred_element_type=F32)


def dot_t(a, b):
    return lax.dot_general(a, b, (((1,), (1,)), ((), ())), preferred_element_type=F32)


def kernel(
    tok, ids, gws, sg, su, sd, eg, eu, ed, out,
    wp, mine, mg, tblk, outw, outg, full, wg, wu, wd, pbuf, r1, sbuf, keep, r2, fin, ret, zout, zin,
    whi, wlo, own, wall,
    mg_s, mg_r, tp_s, th_s, dw_s, dw_r, dp_s, dp_r, tc_s, tc_r, td_s, td_r,
    ds_s, ds_r, a1_s, a1_r, a2_s, a2_r, b_s, b_r, r1_s, r1_r, r2_s, r2_r, rt_s, rt_r, zr_s, zr_r,
    w0_s, w0_r, zc_s, zc_r, zd_s, zd_r, xp_s, xp_r, xm_s, xm_r, xf_s, xf_r, xg_s, xg_r, l_s,
):
    w = lax.axis_index("wide")
    n = lax.axis_index("narrow")
    x, yh, z = w // (NY * NZ), (w // NZ) % NY, w % NZ
    a, c = n // 2, n % 2

    def dev(xx, yy, zz):
        return ((xx % NX) * NY + yy % NY) * NZ + zz % NZ

    mate = (w, 2 * a + 1 - c)
    over = (w, 2 * (1 - a) + c)
    n_mate, n_over, n_diag = mate[1], over[1], 2 * (1 - a) + 1 - c
    partner = (dev(x, yh + 1, z), n)

    def peer(dx, dy, back=False):
        if back:
            dx, dy = NX - dx, NY - dy
        return (dev(x + dx, yh + dy, z), n if dy % NY == 0 else n_over)

    def remote(src, dst, ssem, rsem, device):
        return pltpu.make_async_remote_copy(
            src_ref=src, dst_ref=dst, send_sem=ssem, recv_sem=rsem,
            device_id=device, device_id_type=MESH,
        )

    def wait(ref, sem):
        pltpu.make_async_copy(ref, ref, sem).wait()

    barrier = pltpu.get_barrier_semaphore()
    friends = [peer(j % NX, j // NX) for j in range(1, GROUPS)]
    friends += [(dev(x, yh, z + dz), n) for dz in range(1, NZ)]
    friends += [mate, over, partner]
    for friend in friends:
        pl.semaphore_signal(barrier, inc=1, device_id=friend, device_id_type=MESH)

    loads = (
        pltpu.make_async_copy(eg.at[0], wg, l_s.at[0]),
        pltpu.make_async_copy(eu.at[0], wu, l_s.at[1]),
        pltpu.make_async_copy(ed.at[0], wd, l_s.at[2]),
    )
    for load in loads:
        load.start()

    for k, shard in enumerate((sg, su, sd)):
        for half in range(NY):
            wp[half, k] = shard[:, half * H : (half + 1) * H]
    wall[x, z, yh] = wp[yh]
    quarter = pl.ds(pl.multiple_of(n * Q, Q), Q)
    tblk[z] = tok[:, quarter]
    mine[:6] = ids[...].astype(F32)
    mine[8:14] = gws[...]
    mg[z] = mine[...]
    upper = jnp.where(
        lax.broadcasted_iota(jnp.int32, (TOK, TOK), 0)
        < lax.broadcasted_iota(jnp.int32, (TOK, TOK), 1),
        1.0, 0.0,
    ).astype(BF16)
    row = lax.broadcasted_iota(jnp.int32, (ROWS, GROUPS), 0) // CAP
    spread = jnp.where(
        (((x + row % NX) % NX) * NY + (yh + row // NX) % NY)
        == lax.broadcasted_iota(jnp.int32, (ROWS, GROUPS), 1),
        1.0, 0.0,
    ).astype(BF16)
    slot = (lax.broadcasted_iota(jnp.int32, (ROWS, TOK), 0) % CAP).astype(F32)
    expert = (lax.broadcasted_iota(jnp.int32, (GROUPS, TOK), 0) * NZ + z).astype(F32)

    pl.semaphore_wait(barrier, len(friends))

    w0 = remote(wp.at[1 - yh], wall.at[x, z, yh], w0_s, w0_r, partner)
    w0.start()

    def meta_send(dz):
        return remote(mine, mg.at[z], mg_s, mg_r.at[dz], (dev(x, yh, z + dz), n))

    def block(dz):
        return tblk.at[(z + dz) % NZ]

    def token_send(s):
        up, down = block(NZ - s), block(s)
        up_src, down_src = up, down
        if s == 0:
            up_src = down_src = tok.at[:, quarter]
        if s == 3:
            up_src = up = up.at[: TOK // 2]
            down_src = down = down.at[TOK // 2 :]
        return (
            remote(up_src, up, tc_s.at[s], tc_r.at[s], (dev(x, yh, z + 1), n)),
            remote(down_src, down, td_s.at[s], td_r.at[s], (dev(x, yh, z + NZ - 1), n)),
        )

    def token_ring(s):
        if s < 4:
            wait(block(NZ - s), tc_r.at[s - 1])
            wait(block(s), td_r.at[s - 1])
            for copy in token_send(s):
                copy.start()
        else:
            wait(block(4).at[: TOK // 2], tc_r.at[3])
            wait(block(4).at[TOK // 2 :], td_r.at[3])

    for copy in token_send(0):
        copy.start()
    for dz in range(1, NZ):
        meta_send(dz).start()
    other_quarter = pl.ds(pl.multiple_of(n_over * Q, Q), Q)
    to_partner = (
        remote(
            tok.at[:, quarter], full.at[GROUPS, n_over],
            tp_s, ds_r.at[GROUPS], (partner[0], n_over),
        ),
        remote(tok.at[:, other_quarter], full.at[GROUPS, n], dp_s, dp_r, (partner[0], n_over)),
    )

    def offset(k):
        steps = [(k + GROUPS - j) // GROUPS * (ORDER[j] - ORDER[j - 1]) for j in range(1, GROUPS)]
        return ORDER[0] + sum(steps)

    def part_of(j):
        return pl.ds(j * CAP, CAP)

    def row_send(k, j):
        return remote(
            outg.at[k, part_of(j)], full.at[k, peer(j % NX, j // NX)[1], part_of(j)],
            ds_s, ds_r.at[k], peer(j % NX, j // NX),
        )

    def row_send_wide(j):
        target = peer(j % NX, j // NX)
        return remote(
            outw.at[part_of(j)], full.at[0, n_over if j < NX else n, part_of(j)],
            dw_s, dw_r, target,
        )

    def select(k):
        zb = (z + offset(k)) % NZ
        if k > 0:
            wait(mg.at[zb], mg_r.at[(NZ - offset(k)) % NZ])
        named = jnp.zeros((GROUPS, TOK), F32)
        weight = jnp.zeros((GROUPS, TOK), F32)
        for t in range(6):
            hit = mg[zb, t : t + 1, :] == expert
            named = jnp.where(hit, 1.0, named)
            weight = jnp.where(hit, mg[zb, 8 + t : 9 + t, :], weight)
        before = dot(named.astype(BF16), upper)
        rank = jnp.where(named > 0.0, before, -1.0)
        hit = dot(spread, rank.astype(BF16)) == slot
        pick = jnp.where(hit, 1.0, 0.0).astype(BF16)
        outg[k] = dot(pick, tblk[zb]).astype(BF16)
        for j in range(1, GROUPS):
            row_send(k, j).start()
        full[k, n, :CAP] = outg[k, :CAP]
        if k == 0:
            outw[...] = dot(pick, tok[:, other_quarter]).astype(BF16)
            for j in range(1, GROUPS):
                row_send_wide(j).start()
            full[0, n_over, :CAP] = outw[:CAP]
        w_hi = weight.astype(BF16)
        w_lo = (weight - w_hi.astype(F32)).astype(BF16)
        zero = jnp.zeros((ROWS, TOK), F32)
        whi[k] = jnp.where(hit, dot(spread, w_hi), zero).T.astype(BF16)
        wlo[k] = jnp.where(hit, dot(spread, w_lo), zero).T.astype(BF16)

    def unit(xx, dz):
        return wall.at[xx % NX, (z + dz) % NZ]

    def x_send(dz):
        u = unit(x, dz)
        return (
            remote(u, u, xp_s, xp_r.at[dz], (dev(x + 1, yh, z), n)),
            remote(u, u, xm_s, xm_r.at[dz], (dev(x + NX - 1, yh, z), n)),
        )

    def x_forward(dz):
        lower = unit(x + NX - 1, dz).at[0]
        upper = unit(x + 1, dz).at[1]
        return (
            remote(lower, lower, xf_s, xf_r, (dev(x + 1, yh, z), n)),
            remote(upper, upper, xg_s, xg_r, (dev(x + NX - 1, yh, z), n)),
        )

    def z_send(s):
        up, down = unit(x, NZ - s), unit(x, s)
        if s == 3:
            up, down = up.at[0], down.at[1]
        return (
            remote(up, up, zc_s.at[s], zc_r.at[s], (dev(x, yh, z + 1), n)),
            remote(down, down, zd_s.at[s], zd_r.at[s], (dev(x, yh, z + NZ - 1), n)),
        )

    def ring(s):
        if s == 0:
            wait(wall.at[x, z, 1 - yh], w0_r)
        elif s < 4:
            wait(unit(x, NZ - s), zc_r.at[s - 1])
            wait(unit(x, s), zd_r.at[s - 1])
        else:
            wait(unit(x, 4).at[0], zc_r.at[3])
            wait(unit(x, 4).at[1], zd_r.at[3])
        if s < 4:
            for copy in z_send(s):
                copy.start()

    def forward(dz):
        wait(unit(x + NX - 1, dz), xp_r.at[dz])
        wait(unit(x + 1, dz), xm_r.at[dz])
        for copy in x_forward(dz):
            copy.start()

    for load in loads:
        load.wait()

    def gather_mate(i):
        return remote(full.at[i, n], full.at[i, n], a1_s, a1_r.at[i], mate)

    def gather_over(i):
        return remote(full.at[i, n], full.at[i, n], a2_s, a2_r.at[i], over)

    def gather_diag(i):
        return remote(full.at[i, n_over], full.at[i, n_over], b_s, b_r.at[i], mate)

    def scatter_mate(i):
        return remote(pbuf.at[i, 1 - c], r1.at[i], r1_s, r1_r.at[i], mate)

    def scatter_over(i):
        return remote(sbuf.at[i], r2.at[i], r2_s, r2_r.at[i], over)

    def return_copy(k, j):
        return remote(
            fin.at[k, part_of(j)], ret.at[k, part_of(j)],
            rt_s, rt_r.at[k], peer(j % NX, j // NX, back=True),
        )

    to_home = remote(
        fin.at[GROUPS], ret.at[GROUPS], th_s, rt_r.at[GROUPS],
        (partner[0], n_over),
    )

    def arrive(i):
        if i < GROUPS:
            wait(full.at[i, n, pl.ds(CAP, ROWS - CAP)], ds_r.at[i])
        else:
            wait(full.at[GROUPS, n], ds_r.at[GROUPS])
            wait(full.at[GROUPS, n_over], dp_r)
        if i == 0:
            wait(full.at[0, n_over, pl.ds(CAP, ROWS - CAP)], dw_r)
        if i in (0, GROUPS):
            gather_diag(i).start()
        else:
            gather_over(i).start()
        gather_mate(i).start()

    def pass_on(i):
        wait(full.at[i, n_over], a2_r.at[i])
        gather_diag(i).start()

    def gathered(i):
        wait(full.at[i, n_mate], a1_r.at[i])
        wait(full.at[i, n_diag], b_r.at[i])

    half = ROWS // 2

    def ffn(i):
        gathered(i)
        gp = jnp.zeros((ROWS, H), F32)
        up = jnp.zeros((ROWS, H), F32)
        for q in range(4):
            rows = jnp.concatenate([full[i, q, :half], full[i, (q + 2) % 4, half:]], axis=0)
            gp += dot_t(rows, wg[:, q * Q : (q + 1) * Q])
            up += dot_t(rows, wu[:, q * Q : (q + 1) * Q])
        hidden = silu_mul(gp, up)
        for q in range(4):
            part = dot(hidden, wd[:, q * Q : (q + 1) * Q]).astype(BF16)
            pbuf[i, q % 2, q // 2, :half] = part[:half]
            pbuf[i, q % 2, 1 - q // 2, half:] = part[half:]
        scatter_mate(i).start()

    def add_mate(i):
        wait(r1.at[i], r1_r.at[i])
        sbuf[i] = (pbuf[i, c, 1 - a].astype(F32) + r1[i, 1 - a].astype(F32)).astype(BF16)
        scatter_over(i).start()
        keep[i] = pbuf[i, c, a].astype(F32) + r1[i, a].astype(F32)

    def add_over(i):
        wait(r2.at[i], r2_r.at[i])
        return keep[i] + r2[i].astype(F32)

    def send_home(i):
        fin[i] = add_over(i).astype(BF16)
        for j in range(1, GROUPS):
            return_copy(i, j).start()
        ret[i, :CAP] = fin[i, :CAP]

    def z_return(k):
        return remote(
            zout.at[k], zin.at[k], zr_s, zr_r.at[k], (dev(x, yh, z + offset(k)), n)
        )

    def combine(k):
        wait(ret.at[k, pl.ds(CAP, ROWS - CAP)], rt_r.at[k])
        part = dot(whi[k], ret[k]) + dot(wlo[k], ret[k])

        @pl.when(k == 0)
        def _():
            own[...] = part

        @pl.when(k > 0)
        def _():
            zout[k] = part.astype(BF16)
            z_return(k).start()

    def shared():
        wait(wall.at[0, : NZ // 2], xf_r)
        wait(wall.at[0, : NZ // 2], xg_r)
        gathered(GROUPS)
        gp = jnp.zeros((2 * TOK, H), F32)
        up = jnp.zeros((2 * TOK, H), F32)
        wide_block = NZ * 32
        for k in range(NX * NY):
            xx, yy = k // NY, k % NY
            rows = jnp.concatenate(
                [
                    full[GROUPS, (xx + 2) % 4, :, yy * wide_block : (yy + 1) * wide_block],
                    tok[:, k * wide_block : (k + 1) * wide_block],
                ],
                axis=0,
            )
            gp += dot(rows, wall[xx, :, yy, 0].reshape(wide_block, H))
            up += dot(rows, wall[xx, :, yy, 1].reshape(wide_block, H))
        hidden = silu_mul(gp, up)
        for k in range(NX * NY):
            xx, yy = k // NY, k % NY
            part = dot_t(hidden, wall[xx, :, yy, 2].reshape(wide_block, H)).astype(BF16)
            cols = slice(yy * wide_block, (yy + 1) * wide_block)
            pbuf[GROUPS, xx % 2, 1 - xx // 2, :, cols] = part[:TOK]
            pbuf[GROUPS + 1, xx % 2, xx // 2, :, cols] = part[TOK:]
        scatter_mate(GROUPS).start()
        scatter_mate(GROUPS + 1).start()

    side = {}
    for its, job in (
        (TOKEN_RING, lambda k: token_ring(k + 1)),
        (SELECT, select),
        (ARRIVE, arrive),
        (PASS_ON, lambda k: pass_on(k + 1)),
    ):
        for k, it in enumerate(its):
            side.setdefault(it, []).append((job, k))
    late = {}
    for its, job in (
        (RING, ring),
        (X_SEND, lambda k: [copy.start() for copy in x_send(UNITS[k])]),
        (FORWARD, lambda k: forward(UNITS[k])),
        ((PARTNER,), lambda k: [copy.start() for copy in to_partner]),
        ((SHARED,), lambda k: shared()),
        ((SHARED + 1,) * 2, lambda k: add_mate(GROUPS + k)),
    ):
        for k, it in enumerate(its):
            late.setdefault(it, []).append((job, k))

    def run(jobs, i):
        for it, todo in jobs.items():
            @pl.when(i == it)
            def _():
                for job, k in todo:
                    job(k)

    def step(i, carry):
        run(side, i)
        for first, lag, stage in zip(FIRST, LAG, (ffn, add_mate, send_home, combine)):
            @pl.when((i == first) | ((i > lag) & (i < GROUPS + lag)))
            def _():
                stage((i - lag) * ((i + 63 - lag) // 64))

        run(late, i)
        return carry

    lax.fori_loop(0, GROUPS + LAG[3], step, 0)

    fin[GROUPS] = add_over(GROUPS).astype(BF16)
    to_home.start()
    acc = own[...]
    for k in range(1, GROUPS):
        wait(zin.at[k], zr_r.at[k])
        acc += zin[k].astype(F32)
    acc = acc + add_over(GROUPS + 1)
    wait(ret.at[GROUPS], rt_r.at[GROUPS])
    out[...] = (acc + ret[GROUPS].astype(F32)).astype(BF16)

    w0.wait_send()
    for copy in to_partner:
        copy.wait_send()
    to_home.wait_send()
    wait(outg.at[: GROUPS - 1], ds_s)
    wait(outg.at[: GROUPS - 1], rt_s)
    wait(outg.at[: GROUPS - 1], zr_s)
    wait(mg.at[: NZ - 1], mg_s)
    wait(full.at[:, 0], a1_s)
    wait(full.at[: GROUPS - 1, 0], a2_s)
    wait(full.at[:, 0], b_s)
    wait(outg.at[0, : ROWS - CAP], dw_s)
    wait(r1, r1_s)
    wait(r2, r2_s)
    wait(wall.at[0], xp_s)
    wait(wall.at[0], xm_s)
    wait(wall.at[0, : NZ // 2], xf_s)
    wait(wall.at[0, : NZ // 2], xg_s)
    for s in range(4):
        for copy in token_send(s) + z_send(s):
            copy.wait_send()


def layer(tok, ids, gws, sg, su, sd, eg, eu, ed):
    vmem = pl.BlockSpec(memory_space=pltpu.VMEM)
    hbm = pl.BlockSpec(memory_space=pl.ANY)
    dma = pltpu.SemaphoreType.DMA
    G = GROUPS
    return pl.pallas_call(
        kernel,
        out_shape=jax.ShapeDtypeStruct((TOK, Q), BF16),
        in_specs=[vmem] * 6 + [hbm] * 3,
        out_specs=vmem,
        scratch_shapes=[
            pltpu.VMEM((NY, 3, 32, H), BF16),
            pltpu.VMEM((16, TOK), F32),
            pltpu.VMEM((NZ, 16, TOK), F32),
            pltpu.VMEM((NZ, TOK, Q), BF16),
            pltpu.VMEM((ROWS, Q), BF16),
            pltpu.VMEM((G, ROWS, Q), BF16),
            pltpu.VMEM((G + 1, 4, ROWS, Q), BF16),
            pltpu.VMEM((H, D), BF16),
            pltpu.VMEM((H, D), BF16),
            pltpu.VMEM((H, D), BF16),
            pltpu.VMEM((G + 2, 2, 2, ROWS, Q), BF16),
            pltpu.VMEM((G + 2, 2, ROWS, Q), BF16),
            pltpu.VMEM((G + 2, ROWS, Q), BF16),
            pltpu.VMEM((G + 2, ROWS, Q), F32),
            pltpu.VMEM((G + 2, ROWS, Q), BF16),
            pltpu.VMEM((G + 1, ROWS, Q), BF16),
            pltpu.VMEM((G + 1, ROWS, Q), BF16),
            pltpu.VMEM((G, TOK, Q), BF16),
            pltpu.VMEM((G, TOK, Q), BF16),
            pltpu.VMEM((G, TOK, ROWS), BF16),
            pltpu.VMEM((G, TOK, ROWS), BF16),
            pltpu.VMEM((TOK, Q), F32),
            pltpu.VMEM((NX, NZ, NY, 3, 32, H), BF16),
            dma, dma((NZ,)), dma, dma, dma, dma, dma, dma,
            dma((4,)), dma((4,)), dma((4,)), dma((4,)),
            dma, dma((G + 1,)), dma, dma((G + 1,)), dma, dma((G + 1,)), dma, dma((G + 1,)),
            dma, dma((G + 2,)), dma, dma((G + 2,)), dma, dma((G + 1,)), dma, dma((G,)),
            dma, dma, dma((4,)), dma((4,)), dma((4,)), dma((4,)),
            dma, dma((NZ,)), dma, dma((NZ,)), dma, dma, dma, dma,
            dma((3,)),
        ],
        compiler_params=pltpu.CompilerParams(
            collective_id=0, has_side_effects=True, vmem_limit_bytes=62 * 1024 * 1024
        ),
    )(tok, ids, gws, sg, su, sd, eg, eu, ed)


def body(tokens, expert_ids, gate_weights, shared_gate, shared_up, shared_down,
         expert_gate, expert_up, expert_down):
    return layer(
        tokens, expert_ids.T, gate_weights.T, shared_gate, shared_up, shared_down.T,
        jnp.swapaxes(expert_gate, 1, 2), jnp.swapaxes(expert_up, 1, 2), expert_down,
    )


def solution(mesh):
    in_specs = (
        P("wide", None), P("wide", None), P("wide", None),
        P("wide", "narrow"), P("wide", "narrow"), P("narrow", "wide"),
        P("wide", None, "narrow"), P("wide", None, "narrow"), P("wide", "narrow", None),
    )
    return jax.shard_map(
        body, mesh=mesh, in_specs=in_specs, out_specs=P("wide", "narrow"), check_vma=False
    )
```

```python
import jax
import jax.numpy as jnp
from jax import lax
from jax.experimental import pallas as pl
from jax.experimental.pallas import tpu as pltpu
from jax.sharding import PartitionSpec as P

MESH = pl.DeviceIdType.MESH
BF16 = jnp.bfloat16
F32 = jnp.float32

NX, NY, NZ = 4, 2, 8
CAP = 16
GROUPS = NX * NY
ROWS = NZ * CAP
TOK = 128
D = 2048
Q = D // 4
H = 352
ORDER = (0, 7, 1, 6, 2, 5, 3, 4)
UNITS = (0, 7, 1, 6, 2, 5, 3, 4)
ORDER = (0, 7, 6, 4, 3, 5, 2, 1)
TOKEN_RING = (2, 4, 5, 6)
SELECT = (0, 2, 4, 6, 5, 5, 4, 2)
ARRIVE = (1, 4, 5, 7, 6, 6, 5, 4, 7)
PASS_ON = (5, 6, 8, 7, 7, 6, 5)
FIRST = (3, 4, 5, 7)
LAG = (5, 6, 7, 8)
RING = (2, 4, 5, 6, 8)
X_SEND = (2, 4, 5, 6, 7, 8, 9, 10)
FORWARD = (5, 7, 8, 9, 10, 11, 12, 13)
SHARED = 14
PARTNER = 4


def silu_mul(g, u):
    return (g * jax.nn.sigmoid(g) * u).astype(BF16)


def dot(a, b):
    return jnp.dot(a, b, preferred_element_type=F32)


def dot_t(a, b):
    return lax.dot_general(a, b, (((1,), (1,)), ((), ())), preferred_element_type=F32)


def kernel(
    tok, ids, gws, sg, su, sd, eg, eu, ed, out,
    wp, mine, mg, tblk, outw, outg, full, wg, wu, wd, pbuf, r1, sbuf, keep, r2, fin, ret, zout, zin,
    whi, wlo, own, wall,
    mg_s, mg_r, tp_s, th_s, dw_s, dw_r, dp_s, dp_r, tc_s, tc_r, td_s, td_r,
    ds_s, ds_r, a1_s, a1_r, a2_s, a2_r, b_s, b_r, r1_s, r1_r, r2_s, r2_r, rt_s, rt_r, zr_s, zr_r,
    w0_s, w0_r, zc_s, zc_r, zd_s, zd_r, xp_s, xp_r, xm_s, xm_r, xf_s, xf_r, xg_s, xg_r, l_s,
):
    w = lax.axis_index("wide")
    n = lax.axis_index("narrow")
    x, yh, z = w // (NY * NZ), (w // NZ) % NY, w % NZ
    a, c = n // 2, n % 2

    def dev(xx, yy, zz):
        return ((xx % NX) * NY + yy % NY) * NZ + zz % NZ

    mate = (w, 2 * a + 1 - c)
    over = (w, 2 * (1 - a) + c)
    n_mate, n_over, n_diag = mate[1], over[1], 2 * (1 - a) + 1 - c
    partner = (dev(x, yh + 1, z), n)

    def peer(dx, dy, back=False):
        if back:
            dx, dy = NX - dx, NY - dy
        return (dev(x + dx, yh + dy, z), n if dy % NY == 0 else n_over)

    def remote(src, dst, ssem, rsem, device):
        return pltpu.make_async_remote_copy(
            src_ref=src, dst_ref=dst, send_sem=ssem, recv_sem=rsem,
            device_id=device, device_id_type=MESH,
        )

    def wait(ref, sem):
        pltpu.make_async_copy(ref, ref, sem).wait()

    barrier = pltpu.get_barrier_semaphore()
    friends = [peer(j % NX, j // NX) for j in range(1, GROUPS)]
    friends += [(dev(x, yh, z + dz), n) for dz in range(1, NZ)]
    friends += [mate, over, partner]
    for friend in friends:
        pl.semaphore_signal(barrier, inc=1, device_id=friend, device_id_type=MESH)

    loads = (
        pltpu.make_async_copy(eg.at[0], wg, l_s.at[0]),
        pltpu.make_async_copy(eu.at[0], wu, l_s.at[1]),
        pltpu.make_async_copy(ed.at[0], wd, l_s.at[2]),
    )
    for load in loads:
        load.start()

    for k, shard in enumerate((sg, su, sd)):
        for half in range(NY):
            wp[half, k] = shard[:, half * H : (half + 1) * H]
    wall[x, z, yh] = wp[yh]
    quarter = pl.ds(pl.multiple_of(n * Q, Q), Q)
    tblk[z] = tok[:, quarter]
    mine[:6] = ids[...].astype(F32)
    mine[8:14] = gws[...]
    mg[z] = mine[...]
    upper = jnp.where(
        lax.broadcasted_iota(jnp.int32, (TOK, TOK), 0)
        < lax.broadcasted_iota(jnp.int32, (TOK, TOK), 1),
        1.0, 0.0,
    ).astype(BF16)
    row = lax.broadcasted_iota(jnp.int32, (ROWS, GROUPS), 0) // CAP
    spread = jnp.where(
        (((x + row % NX) % NX) * NY + (yh + row // NX) % NY)
        == lax.broadcasted_iota(jnp.int32, (ROWS, GROUPS), 1),
        1.0, 0.0,
    ).astype(BF16)
    slot = (lax.broadcasted_iota(jnp.int32, (ROWS, TOK), 0) % CAP).astype(F32)
    expert = (lax.broadcasted_iota(jnp.int32, (GROUPS, TOK), 0) * NZ + z).astype(F32)

    pl.semaphore_wait(barrier, len(friends))

    w0 = remote(wp.at[1 - yh], wall.at[x, z, yh], w0_s, w0_r, partner)
    w0.start()

    def meta_send(dz):
        return remote(mine, mg.at[z], mg_s, mg_r.at[dz], (dev(x, yh, z + dz), n))

    def block(dz):
        return tblk.at[(z + dz) % NZ]

    def token_send(s):
        up, down = block(NZ - s), block(s)
        up_src, down_src = up, down
        if s == 0:
            up_src = down_src = tok.at[:, quarter]
        if s == 3:
            up_src = up = up.at[: TOK // 2]
            down_src = down = down.at[TOK // 2 :]
        return (
            remote(up_src, up, tc_s.at[s], tc_r.at[s], (dev(x, yh, z + 1), n)),
            remote(down_src, down, td_s.at[s], td_r.at[s], (dev(x, yh, z + NZ - 1), n)),
        )

    def token_ring(s):
        if s < 4:
            wait(block(NZ - s), tc_r.at[s - 1])
            wait(block(s), td_r.at[s - 1])
            for copy in token_send(s):
                copy.start()
        else:
            wait(block(4).at[: TOK // 2], tc_r.at[3])
            wait(block(4).at[TOK // 2 :], td_r.at[3])

    for copy in token_send(0):
        copy.start()
    for dz in range(1, NZ):
        meta_send(dz).start()
    other_quarter = pl.ds(pl.multiple_of(n_over * Q, Q), Q)
    to_partner = (
        remote(
            tok.at[:, quarter], full.at[GROUPS, n_over],
            tp_s, ds_r.at[GROUPS], (partner[0], n_over),
        ),
        remote(tok.at[:, other_quarter], full.at[GROUPS, n], dp_s, dp_r, (partner[0], n_over)),
    )

    def offset(k):
        steps = [(k + GROUPS - j) // GROUPS * (ORDER[j] - ORDER[j - 1]) for j in range(1, GROUPS)]
        return ORDER[0] + sum(steps)

    def part_of(j):
        return pl.ds(j * CAP, CAP)

    def row_send(k, j):
        return remote(
            outg.at[k, part_of(j)], full.at[k, peer(j % NX, j // NX)[1], part_of(j)],
            ds_s, ds_r.at[k], peer(j % NX, j // NX),
        )

    def row_send_wide(j):
        target = peer(j % NX, j // NX)
        return remote(
            outw.at[part_of(j)], full.at[0, n_over if j < NX else n, part_of(j)],
            dw_s, dw_r, target,
        )

    def select(k):
        zb = (z + offset(k)) % NZ
        if k > 0:
            wait(mg.at[zb], mg_r.at[(NZ - offset(k)) % NZ])
        named = jnp.zeros((GROUPS, TOK), F32)
        weight = jnp.zeros((GROUPS, TOK), F32)
        for t in range(6):
            hit = mg[zb, t : t + 1, :] == expert
            named = jnp.where(hit, 1.0, named)
            weight = jnp.where(hit, mg[zb, 8 + t : 9 + t, :], weight)
        before = dot(named.astype(BF16), upper)
        rank = jnp.where(named > 0.0, before, -1.0)
        hit = dot(spread, rank.astype(BF16)) == slot
        pick = jnp.where(hit, 1.0, 0.0).astype(BF16)
        outg[k] = dot(pick, tblk[zb]).astype(BF16)
        for j in range(1, GROUPS):
            row_send(k, j).start()
        full[k, n, :CAP] = outg[k, :CAP]
        if k == 0:
            outw[...] = dot(pick, tok[:, other_quarter]).astype(BF16)
            for j in range(1, GROUPS):
                row_send_wide(j).start()
            full[0, n_over, :CAP] = outw[:CAP]
        w_hi = weight.astype(BF16)
        w_lo = (weight - w_hi.astype(F32)).astype(BF16)
        zero = jnp.zeros((ROWS, TOK), F32)
        whi[k] = jnp.where(hit, dot(spread, w_hi), zero).T.astype(BF16)
        wlo[k] = jnp.where(hit, dot(spread, w_lo), zero).T.astype(BF16)

    def unit(xx, dz):
        return wall.at[xx % NX, (z + dz) % NZ]

    def x_send(dz):
        u = unit(x, dz)
        return (
            remote(u, u, xp_s, xp_r.at[dz], (dev(x + 1, yh, z), n)),
            remote(u, u, xm_s, xm_r.at[dz], (dev(x + NX - 1, yh, z), n)),
        )

    def x_forward(dz):
        lower = unit(x + NX - 1, dz).at[0]
        upper = unit(x + 1, dz).at[1]
        return (
            remote(lower, lower, xf_s, xf_r, (dev(x + 1, yh, z), n)),
            remote(upper, upper, xg_s, xg_r, (dev(x + NX - 1, yh, z), n)),
        )

    def z_send(s):
        up, down = unit(x, NZ - s), unit(x, s)
        if s == 3:
            up, down = up.at[0], down.at[1]
        return (
            remote(up, up, zc_s.at[s], zc_r.at[s], (dev(x, yh, z + 1), n)),
            remote(down, down, zd_s.at[s], zd_r.at[s], (dev(x, yh, z + NZ - 1), n)),
        )

    def ring(s):
        if s == 0:
            wait(wall.at[x, z, 1 - yh], w0_r)
        elif s < 4:
            wait(unit(x, NZ - s), zc_r.at[s - 1])
            wait(unit(x, s), zd_r.at[s - 1])
        else:
            wait(unit(x, 4).at[0], zc_r.at[3])
            wait(unit(x, 4).at[1], zd_r.at[3])
        if s < 4:
            for copy in z_send(s):
                copy.start()

    def forward(dz):
        wait(unit(x + NX - 1, dz), xp_r.at[dz])
        wait(unit(x + 1, dz), xm_r.at[dz])
        for copy in x_forward(dz):
            copy.start()

    for load in loads:
        load.wait()

    def gather_mate(i):
        return remote(full.at[i, n], full.at[i, n], a1_s, a1_r.at[i], mate)

    def gather_over(i):
        return remote(full.at[i, n], full.at[i, n], a2_s, a2_r.at[i], over)

    def gather_diag(i):
        return remote(full.at[i, n_over], full.at[i, n_over], b_s, b_r.at[i], mate)

    def scatter_mate(i):
        return remote(pbuf.at[i, 1 - c], r1.at[i], r1_s, r1_r.at[i], mate)

    def scatter_over(i):
        return remote(sbuf.at[i], r2.at[i], r2_s, r2_r.at[i], over)

    def return_copy(k, j):
        return remote(
            fin.at[k, part_of(j)], ret.at[k, part_of(j)],
            rt_s, rt_r.at[k], peer(j % NX, j // NX, back=True),
        )

    to_home = remote(
        fin.at[GROUPS], ret.at[GROUPS], th_s, rt_r.at[GROUPS],
        (partner[0], n_over),
    )

    def arrive(i):
        if i < GROUPS:
            wait(full.at[i, n, pl.ds(CAP, ROWS - CAP)], ds_r.at[i])
        else:
            wait(full.at[GROUPS, n], ds_r.at[GROUPS])
            wait(full.at[GROUPS, n_over], dp_r)
        if i == 0:
            wait(full.at[0, n_over, pl.ds(CAP, ROWS - CAP)], dw_r)
        if i in (0, GROUPS):
            gather_diag(i).start()
        else:
            gather_over(i).start()
        gather_mate(i).start()

    def pass_on(i):
        wait(full.at[i, n_over], a2_r.at[i])
        gather_diag(i).start()

    def gathered(i):
        wait(full.at[i, n_mate], a1_r.at[i])
        wait(full.at[i, n_diag], b_r.at[i])

    half = ROWS // 2

    def ffn(i):
        gathered(i)
        gp = jnp.zeros((ROWS, H), F32)
        up = jnp.zeros((ROWS, H), F32)
        for q in range(4):
            rows = jnp.concatenate([full[i, q, :half], full[i, (q + 2) % 4, half:]], axis=0)
            gp += dot_t(rows, wg[:, q * Q : (q + 1) * Q])
            up += dot_t(rows, wu[:, q * Q : (q + 1) * Q])
        hidden = silu_mul(gp, up)
        for q in range(4):
            part = dot(hidden, wd[:, q * Q : (q + 1) * Q]).astype(BF16)
            pbuf[i, q % 2, q // 2, :half] = part[:half]
            pbuf[i, q % 2, 1 - q // 2, half:] = part[half:]
        scatter_mate(i).start()

    def add_mate(i):
        wait(r1.at[i], r1_r.at[i])
        sbuf[i] = (pbuf[i, c, 1 - a].astype(F32) + r1[i, 1 - a].astype(F32)).astype(BF16)
        scatter_over(i).start()
        keep[i] = pbuf[i, c, a].astype(F32) + r1[i, a].astype(F32)

    def add_over(i):
        wait(r2.at[i], r2_r.at[i])
        return keep[i] + r2[i].astype(F32)

    def send_home(i):
        fin[i] = add_over(i).astype(BF16)
        for j in range(1, GROUPS):
            return_copy(i, j).start()
        ret[i, :CAP] = fin[i, :CAP]

    def z_return(k):
        return remote(
            zout.at[k], zin.at[k], zr_s, zr_r.at[k], (dev(x, yh, z + offset(k)), n)
        )

    def combine(k):
        wait(ret.at[k, pl.ds(CAP, ROWS - CAP)], rt_r.at[k])
        part = dot(whi[k], ret[k]) + dot(wlo[k], ret[k])

        @pl.when(k == 0)
        def _():
            own[...] = part

        @pl.when(k > 0)
        def _():
            zout[k] = part.astype(BF16)
            z_return(k).start()

    def shared():
        wait(wall.at[0, : NZ // 2], xf_r)
        wait(wall.at[0, : NZ // 2], xg_r)
        gathered(GROUPS)
        gp = jnp.zeros((2 * TOK, H), F32)
        up = jnp.zeros((2 * TOK, H), F32)
        wide_block = NZ * 32
        for k in range(NX * NY):
            xx, yy = k // NY, k % NY
            rows = jnp.concatenate(
                [
                    full[GROUPS, (xx + 2) % 4, :, yy * wide_block : (yy + 1) * wide_block],
                    tok[:, k * wide_block : (k + 1) * wide_block],
                ],
                axis=0,
            )
            gp += dot(rows, wall[xx, :, yy, 0].reshape(wide_block, H))
            up += dot(rows, wall[xx, :, yy, 1].reshape(wide_block, H))
        hidden = silu_mul(gp, up)
        for k in range(NX * NY):
            xx, yy = k // NY, k % NY
            part = dot_t(hidden, wall[xx, :, yy, 2].reshape(wide_block, H)).astype(BF16)
            cols = slice(yy * wide_block, (yy + 1) * wide_block)
            pbuf[GROUPS, xx % 2, 1 - xx // 2, :, cols] = part[:TOK]
            pbuf[GROUPS + 1, xx % 2, xx // 2, :, cols] = part[TOK:]
        scatter_mate(GROUPS).start()
        scatter_mate(GROUPS + 1).start()

    side = {}
    for its, job in (
        (TOKEN_RING, lambda k: token_ring(k + 1)),
        (SELECT, select),
        (ARRIVE, arrive),
        (PASS_ON, lambda k: pass_on(k + 1)),
        ((SHARED,), lambda k: shared()),
        ((SHARED + 1,) * 2, lambda k: add_mate(GROUPS + k)),
    ):
        for k, it in enumerate(its):
            side.setdefault(it, []).append((job, k))
    late = {}
    for its, job in (
        (RING, ring),
        (X_SEND, lambda k: [copy.start() for copy in x_send(UNITS[k])]),
        (FORWARD, lambda k: forward(UNITS[k])),
        ((PARTNER,), lambda k: [copy.start() for copy in to_partner]),
    ):
        for k, it in enumerate(its):
            late.setdefault(it, []).append((job, k))

    def run(jobs, i):
        for it, todo in jobs.items():
            @pl.when(i == it)
            def _():
                for job, k in todo:
                    job(k)

    def step(i, carry):
        run(side, i)
        for first, lag, stage in zip(FIRST, LAG, (ffn, add_mate, send_home, combine)):
            @pl.when((i == first) | ((i > lag) & (i < GROUPS + lag)))
            def _():
                stage((i - lag) * ((i + 63 - lag) // 64))

        run(late, i)
        return carry

    lax.fori_loop(0, GROUPS + LAG[3], step, 0)

    fin[GROUPS] = add_over(GROUPS).astype(BF16)
    to_home.start()
    acc = own[...]
    for k in range(1, GROUPS):
        wait(zin.at[k], zr_r.at[k])
        acc += zin[k].astype(F32)
    acc = acc + add_over(GROUPS + 1)
    wait(ret.at[GROUPS], rt_r.at[GROUPS])
    out[...] = (acc + ret[GROUPS].astype(F32)).astype(BF16)

    w0.wait_send()
    for copy in to_partner:
        copy.wait_send()
    to_home.wait_send()
    wait(outg.at[: GROUPS - 1], ds_s)
    wait(outg.at[: GROUPS - 1], rt_s)
    wait(outg.at[: GROUPS - 1], zr_s)
    wait(mg.at[: NZ - 1], mg_s)
    wait(full.at[:, 0], a1_s)
    wait(full.at[: GROUPS - 1, 0], a2_s)
    wait(full.at[:, 0], b_s)
    wait(outg.at[0, : ROWS - CAP], dw_s)
    wait(r1, r1_s)
    wait(r2, r2_s)
    wait(wall.at[0], xp_s)
    wait(wall.at[0], xm_s)
    wait(wall.at[0, : NZ // 2], xf_s)
    wait(wall.at[0, : NZ // 2], xg_s)
    for s in range(4):
        for copy in token_send(s) + z_send(s):
            copy.wait_send()


def layer(tok, ids, gws, sg, su, sd, eg, eu, ed):
    vmem = pl.BlockSpec(memory_space=pltpu.VMEM)
    hbm = pl.BlockSpec(memory_space=pl.ANY)
    dma = pltpu.SemaphoreType.DMA
    G = GROUPS
    return pl.pallas_call(
        kernel,
        out_shape=jax.ShapeDtypeStruct((TOK, Q), BF16),
        in_specs=[vmem] * 6 + [hbm] * 3,
        out_specs=vmem,
        scratch_shapes=[
            pltpu.VMEM((NY, 3, 32, H), BF16),
            pltpu.VMEM((16, TOK), F32),
            pltpu.VMEM((NZ, 16, TOK), F32),
            pltpu.VMEM((NZ, TOK, Q), BF16),
            pltpu.VMEM((ROWS, Q), BF16),
            pltpu.VMEM((G, ROWS, Q), BF16),
            pltpu.VMEM((G + 1, 4, ROWS, Q), BF16),
            pltpu.VMEM((H, D), BF16),
            pltpu.VMEM((H, D), BF16),
            pltpu.VMEM((H, D), BF16),
            pltpu.VMEM((G + 2, 2, 2, ROWS, Q), BF16),
            pltpu.VMEM((G + 2, 2, ROWS, Q), BF16),
            pltpu.VMEM((G + 2, ROWS, Q), BF16),
            pltpu.VMEM((G + 2, ROWS, Q), F32),
            pltpu.VMEM((G + 2, ROWS, Q), BF16),
            pltpu.VMEM((G + 1, ROWS, Q), BF16),
            pltpu.VMEM((G + 1, ROWS, Q), BF16),
            pltpu.VMEM((G, TOK, Q), BF16),
            pltpu.VMEM((G, TOK, Q), BF16),
            pltpu.VMEM((G, TOK, ROWS), BF16),
            pltpu.VMEM((G, TOK, ROWS), BF16),
            pltpu.VMEM((TOK, Q), F32),
            pltpu.VMEM((NX, NZ, NY, 3, 32, H), BF16),
            dma, dma((NZ,)), dma, dma, dma, dma, dma, dma,
            dma((4,)), dma((4,)), dma((4,)), dma((4,)),
            dma, dma((G + 1,)), dma, dma((G + 1,)), dma, dma((G + 1,)), dma, dma((G + 1,)),
            dma, dma((G + 2,)), dma, dma((G + 2,)), dma, dma((G + 1,)), dma, dma((G,)),
            dma, dma, dma((4,)), dma((4,)), dma((4,)), dma((4,)),
            dma, dma((NZ,)), dma, dma((NZ,)), dma, dma, dma, dma,
            dma((3,)),
        ],
        compiler_params=pltpu.CompilerParams(
            collective_id=0, has_side_effects=True, vmem_limit_bytes=62 * 1024 * 1024
        ),
    )(tok, ids, gws, sg, su, sd, eg, eu, ed)


def body(tokens, expert_ids, gate_weights, shared_gate, shared_up, shared_down,
         expert_gate, expert_up, expert_down):
    return layer(
        tokens, expert_ids.T, gate_weights.T, shared_gate, shared_up, shared_down.T,
        jnp.swapaxes(expert_gate, 1, 2), jnp.swapaxes(expert_up, 1, 2), expert_down,
    )


def solution(mesh):
    in_specs = (
        P("wide", None), P("wide", None), P("wide", None),
        P("wide", "narrow"), P("wide", "narrow"), P("narrow", "wide"),
        P("wide", None, "narrow"), P("wide", None, "narrow"), P("wide", "narrow", None),
    )
    return jax.shard_map(
        body, mesh=mesh, in_specs=in_specs, out_specs=P("wide", "narrow"), check_vma=False
    )
```
